32 devices in a mesh: head: 4 (over y, x), blk: 8 (over z, core).
Axes of the slice: x: 2, y: 2, z: 4, core: 2. Of those that a mesh axis runs over, the one named last changes fastest.
Arguments:
- hidden_in: bfloat16 [2048, 4096], P(('blk', 'head')), may hold values from -6 to 6
- queries: bfloat16 [2048, 2048], P(('blk', 'head')), may hold values from -26 to 26
- key_states: bfloat16 [2048, 1024], P(('blk', 'head')), may hold values from -5 to 5
- value_states: bfloat16 [2048, 1024], P(('blk', 'head')), may hold values from -6 to 6
- out_weight: bfloat16 [2048, 4096], P('head'), may hold values from -0.125 to 0.125
- norm_gain: float32 [4096], replicated, may hold values from 0.1 to 1.9
- gate_weight: bfloat16 [4096, 7168], P(None, 'head'), may hold values from -0.09375 to 0.09375
- up_weight: bfloat16 [4096, 7168], P(None, 'head'), may hold values from -0.09375 to 0.09375
- down_weight: bfloat16 [7168, 4096], P('head'), may hold values from -0.0625 to 0.0625
Outputs:
- layer_out: bfloat16 [2048, 4096], P(('blk', 'head'))
The draws below stay inside these ranges and needn't reach their ends.
All inputs are finite; a program needn't handle non-finite values.
Results may differ from the reference program's by a relative error of at most 0.018.
Values may be sent and summed in bfloat16 or wider, within the bound.
A program may use at most 192 MiB of HBM per device.

```python
import jax
import jax.numpy as jnp
from jax import lax

D = 4096
HEADS = 16
KV_HEADS = 8
HEAD_DIM = 128
FF = 7168
TOK_BLK = 256
SEQ = 2048


def paired_draw(seed_key):
    anchor = jax.random.fold_in(seed_key, 7)
    stream_keys = jax.random.fold_in(anchor, 1)
    stream_query = jax.random.fold_in(anchor, 2)
    key_width = KV_HEADS * HEAD_DIM
    query_width = HEADS * HEAD_DIM
    key_drawn = jnp.clip(jax.random.normal(stream_keys, (SEQ, key_width), jnp.float32), -5.0, 5.0)
    query_drawn = jnp.clip(2.5 * jax.random.normal(stream_query, (SEQ, query_width), jnp.float32), -15.0, 15.0)
    return (query_drawn, key_drawn)


def draw_queries(key, part):
    return paired_draw(key)[0].astype(jnp.bfloat16)


def draw_key_states(key, part):
    return paired_draw(key)[1].astype(jnp.bfloat16)


def levels(rng, extent, pieces, least, top_value):
    loudness = 1.0
    for axis_at, blocks in pieces:
        heights = jax.random.uniform(jax.random.fold_in(jax.random.fold_in(rng, 6), axis_at), (blocks,), jnp.float32, least / len(pieces), top_value / len(pieces))
        loudness = loudness * jnp.repeat(jnp.exp(heights), extent[axis_at] // blocks).reshape((-1,) + (1,) * (len(extent) - 1 - axis_at))
    return loudness


def normal_values(key, extent, width, reach, pieces=(), held_as=jnp.bfloat16):
    drawn = jax.random.normal(key, extent, jnp.float32) * width
    if len(pieces) > 0:
        drawn = levels(key, extent, pieces, -0.22, 0.18) * drawn
    return jnp.clip(drawn, min=-reach, max=reach).astype(held_as)


def setup_inputs(seed: int = 0) -> dict:
    splits = jax.random.split(jax.random.key(seed), 10)
    return {
        "hidden_in": normal_values(splits[0], (SEQ, D), 1.0, 6.0, ((0, 32),)),
        "queries": draw_queries(jax.random.fold_in(splits[9], 71), 0),
        "key_states": draw_key_states(jax.random.fold_in(splits[9], 71), 0),
        "value_states": normal_values(splits[3], (SEQ, KV_HEADS * HEAD_DIM), 1.0, 6.0, ((0, 32),)),
        "out_weight": normal_values(splits[4], (HEADS * HEAD_DIM, D), (HEADS * HEAD_DIM) ** -0.5, 0.125, ((0, 4),)),
        "norm_gain": jnp.clip(1.0 + 0.18 * jax.random.normal(splits[5], (D,), jnp.float32), 0.1, 1.9),
        "gate_weight": normal_values(splits[6], (D, FF), D ** -0.5, 0.09375, ((1, 4),)),
        "up_weight": normal_values(splits[7], (D, FF), D ** -0.5, 0.09375, ((1, 4),)),
        "down_weight": normal_values(splits[8], (FF, D), FF ** -0.5, 0.0625, ((0, 4),)),
    }


def attend_group(query_group, key_group, value_group):
    score_scale = HEAD_DIM ** (-0.5)
    positions = jnp.arange(SEQ, dtype=jnp.int32)

    def one_block(block_index):
        first_row = block_index * TOK_BLK
        query_block = lax.dynamic_slice_in_dim(query_group, first_row, TOK_BLK, 1)
        scores = jnp.einsum('rqd,kd->rqk', query_block, key_group) * score_scale
        query_pos = first_row + jnp.arange(TOK_BLK, dtype=jnp.int32)
        visible = positions[None, :] <= query_pos[:, None]
        row_peak = lax.optimization_barrier(jnp.max(jnp.where(visible, scores, -jnp.inf), axis=-1))
        exp_scores = jnp.where(visible, jnp.exp(scores - row_peak[..., None]), 0.0)
        row_total = lax.optimization_barrier(jnp.sum(exp_scores, axis=-1))
        rounded = lax.optimization_barrier(exp_scores.astype(jnp.bfloat16)).astype(jnp.float32)
        numerator = jnp.einsum('rqk,kd->rqd', rounded, value_group)
        return (numerator / row_total[..., None]).astype(jnp.bfloat16)
    return lax.map(one_block, jnp.arange(SEQ // TOK_BLK, dtype=jnp.int32))

def attend_tuple(groups):
    return attend_group(groups[0], groups[1], groups[2])

def reference(hidden_in, queries, key_states, value_states, out_weight, norm_gain, gate_weight, up_weight, down_weight):
    group_ratio = HEADS // KV_HEADS
    query_all = queries.astype(jnp.float32).reshape(SEQ, KV_HEADS, group_ratio, HEAD_DIM).transpose(1, 2, 0, 3)
    key_all = key_states.astype(jnp.float32).reshape(SEQ, KV_HEADS, HEAD_DIM).transpose(1, 0, 2)
    value_all = value_states.astype(jnp.float32).reshape(SEQ, KV_HEADS, HEAD_DIM).transpose(1, 0, 2)
    attended = lax.map(attend_tuple, (query_all, key_all, value_all))
    attended = attended.transpose(1, 3, 0, 2, 4).reshape(SEQ, HEADS * HEAD_DIM)
    projected = jnp.dot(attended, out_weight, preferred_element_type=jnp.float32)
    residual = (hidden_in.astype(jnp.float32) + projected).astype(jnp.bfloat16)
    widened = residual.astype(jnp.float32)
    mean_square = lax.optimization_barrier(jnp.mean(widened * widened, axis=-1, keepdims=True))
    normed = (widened * lax.rsqrt(mean_square + 1e-05) * norm_gain.astype(jnp.float32)).astype(jnp.bfloat16)
    gate_part = jnp.dot(normed, gate_weight, preferred_element_type=jnp.float32)
    up_part = jnp.dot(normed, up_weight, preferred_element_type=jnp.float32)
    inner_act = (jax.nn.silu(gate_part) * up_part).astype(jnp.bfloat16)
    mlp_out = jnp.dot(inner_act, down_weight, preferred_element_type=jnp.float32)
    return (residual.astype(jnp.float32) + mlp_out).astype(jnp.bfloat16)
```

```python
import functools

import jax
import jax.numpy as jnp
from jax import lax
from jax.experimental import pallas as pl
from jax.experimental.pallas import tpu as pltpu
from jax.sharding import PartitionSpec as P

HEADS = 16
KV_HEADS = 8
HEAD_DIM = 128
CHUNKS = 4
MESH = pl.DeviceIdType.MESH
BF = jnp.bfloat16
F32 = jnp.float32


def tile_of(n, most=256):
    t = most
    while n % t:
        t -= 128
    return t


def remote(src, dst, send, recv, axis, index):
    return pltpu.make_async_remote_copy(
        src_ref=src, dst_ref=dst, send_sem=send, recv_sem=recv,
        device_id={axis: index}, device_id_type=MESH,
    )


def kernel(
    H, B,
    hid, q_in, k_in, v_in, gain, wo_h, wg_h, wu_h, wd_h,
    out,
    wo, wg, wu, wd, qb, kv, att, part, rs, gath, accg, accu, inner,
    w_sem, loc_sem, a_s, a_r, z_s, z_r, d_s, d_r, rs_s, rs_r, ag_s, ag_r, r2_s, r2_r,
):
    h = lax.axis_index("head")
    b = lax.axis_index("blk")
    J = B // 2
    j = b // 2
    c = b % 2
    partner = b + 1 - 2 * c
    T = hid.shape[0]
    D = hid.shape[1]
    R = T * H
    QW = qb.shape[1]
    KW = kv.shape[3]
    nh = QW // HEAD_DIM
    ratio = HEADS // KV_HEADS
    CW = D // CHUNKS
    FW = wg.shape[1]

    wcopies = [pltpu.make_async_copy(wo_h, wo, w_sem.at[0])]
    for i in range(CHUNKS):
        rows = pl.ds(i * CW, CW)
        wcopies.append(pltpu.make_async_copy(wg_h.at[rows], wg.at[rows], w_sem.at[1 + 2 * i]))
        wcopies.append(pltpu.make_async_copy(wu_h.at[rows], wu.at[rows], w_sem.at[2 + 2 * i]))
    wcopies.append(pltpu.make_async_copy(wd_h, wd, w_sem.at[1 + 2 * CHUNKS]))
    for w in wcopies:
        w.start()

    barrier = pltpu.get_barrier_semaphore()
    for d in range(1, H):
        pl.semaphore_signal(barrier, inc=1, device_id={"head": lax.rem(h + d, H)}, device_id_type=MESH)
    for d in range(1, J):
        pl.semaphore_signal(barrier, inc=1, device_id={"blk": lax.rem(b + 2 * d, B)}, device_id_type=MESH)
    pl.semaphore_signal(barrier, inc=1, device_id={"blk": partner}, device_id_type=MESH)
    pl.semaphore_wait(barrier, H - 1 + J - 1 + 1)

    my_rows = pl.ds(pl.multiple_of(h * T, T), T)

    def cols(p, w):
        return pl.ds(pl.multiple_of(p * w, w), w)

    a_copies = []
    for t, (src, dst, w) in enumerate(
        ((k_in, kv.at[b, 0], KW), (v_in, kv.at[b, 1], KW), (q_in, qb, QW))
    ):
        for d in range(1, H):
            p = lax.rem(h + d, H)
            cp = remote(
                src.at[:, cols(p, w)], dst.at[my_rows, :],
                a_s.at[d - 1, t], a_r.at[d - 1, t], "head", p,
            )
            cp.start()
            a_copies.append((t, cp))
        lc = pltpu.make_async_copy(src.at[:, cols(h, w)], dst.at[my_rows, :], loc_sem.at[t])
        lc.start()
        a_copies.append((t, lc))

    def wait_in(t):
        for tt, cp in a_copies:
            if tt == t:
                cp.wait()

    def z_copy(slot, t):
        return remote(
            kv.at[slot, t], kv.at[slot, t], z_s.at[slot, t], z_r.at[slot, t],
            "blk", lax.rem(b + 2, B),
        )

    def d_copy(slot, t):
        return remote(
            kv.at[slot, t], kv.at[slot, t], d_s.at[slot, t], d_r.at[slot, t], "blk", partner
        )

    for t in range(2):
        wait_in(t)

        @pl.when(j < J - 1)
        def _():
            z_copy(b, t).start()

        @pl.when(c == 0)
        def _():
            d_copy(b, t).start()

    wait_in(2)

    mq = lambda n: slice(n * HEAD_DIM, (n + 1) * HEAD_DIM)
    ml = lambda n: slice((nh + n) * HEAD_DIM, (nh + n + 1) * HEAD_DIM)
    scale = HEAD_DIM ** (-0.5)

    def absorb(slot, first):
        for n in range(nh):
            g = n // ratio
            s = lax.dot_general(
                qb[:, mq(n)], kv[slot, 0, :, mq(g)],
                (((1,), (1,)), ((), ())), preferred_element_type=F32,
            ) * scale
            if first:
                qi = lax.broadcasted_iota(jnp.int32, s.shape, 0)
                ki = lax.broadcasted_iota(jnp.int32, s.shape, 1)
                s = jnp.where(ki <= qi, s, -1e30)
            top = jnp.max(s, axis=1, keepdims=True)
            if not first:
                old = accu[:, mq(n)][:, :1]
                top = jnp.maximum(top, old)
            e = jnp.exp(s - top)
            tot = jnp.sum(e, axis=1, keepdims=True)
            pv = jnp.dot(e.astype(BF), kv[slot, 1, :, mq(g)], preferred_element_type=F32)
            if not first:
                f = jnp.exp(old - top)
                tot = tot + accu[:, ml(n)][:, :1] * f
                pv = pv + accg[:, mq(n)] * f
            accu[:, mq(n)] = jnp.broadcast_to(top, (R, HEAD_DIM))
            accu[:, ml(n)] = jnp.broadcast_to(tot, (R, HEAD_DIM))
            accg[:, mq(n)] = pv

    absorb(b, True)

    @pl.when(c == 1)
    def _():
        for t in range(2):
            d_copy(b - 1, t).wait_recv()
        absorb(b - 1, False)

    def chain(s, carry):
        slot = 2 * (j - 1 - s) + c
        other = 2 * (j - 1 - s) + 1 - c
        for t in range(2):
            z_copy(slot, t).wait_recv()

            @pl.when(j < J - 1)
            def _():
                z_copy(slot, t).start()

            d_copy(slot, t).start()
        absorb(slot, False)
        for t in range(2):
            d_copy(other, t).wait_recv()
        absorb(other, False)
        return carry

    lax.fori_loop(0, j, chain, 0)

    for n in range(nh):
        att[:, mq(n)] = (accg[:, mq(n)] / accu[:, ml(n)]).astype(BF)

    def scatter(w_ref, x_ref, send, recv):
        copies = []
        ct = tile_of(CW)
        for i in range(CHUNKS):
            def step(t, carry):
                cs = pl.ds(pl.multiple_of(i * CW + t * ct, ct), ct)
                part[:, cs] = jnp.dot(
                    x_ref[...], w_ref[:, cs], preferred_element_type=F32
                ).astype(BF)
                return carry

            lax.fori_loop(0, CW // ct, step, 0)
            cs = pl.ds(i * CW, CW)
            for d in range(1, H):
                p = lax.rem(h + d, H)
                cp = remote(
                    part.at[pl.ds(pl.multiple_of(p * T, T), T), cs], rs.at[d - 1, :, cs],
                    send.at[d - 1, i], recv.at[d - 1, i], "head", p,
                )
                cp.start()
                copies.append(cp)
        return copies

    def reduced(i, copies):
        cs = pl.ds(i * CW, CW)
        for d in range(1, H):
            copies[i * (H - 1) + d - 1].wait_recv()
        total = part[my_rows, cs].astype(F32)
        for d in range(1, H):
            total = total + rs[d - 1, :, cs].astype(F32)
        return total

    wcopies[0].wait()
    rs_copies = scatter(wo, att, rs_s, rs_r)
    ag_copies = []
    for i in range(CHUNKS):
        cs = pl.ds(i * CW, CW)
        gath[my_rows, cs] = (hid[:, cs].astype(F32) + reduced(i, rs_copies)).astype(BF)
        for d in range(1, H):
            cp = remote(
                gath.at[my_rows, cs], gath.at[my_rows, cs],
                ag_s.at[d - 1, i], ag_r.at[d - 1, i], "head", lax.rem(h + d, H),
            )
            cp.start()
            ag_copies.append(cp)

    ft = tile_of(FW)
    square = jnp.zeros((R, 1), F32)
    for i in range(CHUNKS):
        cs = pl.ds(i * CW, CW)
        for d in range(1, H):
            ag_copies[i * (H - 1) + d - 1].wait_recv()
        wcopies[1 + 2 * i].wait()
        wcopies[2 + 2 * i].wait()
        x = gath[:, cs].astype(F32)
        square = square + jnp.sum(x * x, axis=1, keepdims=True)
        xg = (x * gain[:, cs]).astype(BF)

        def step(t, carry, xg=xg, cs=cs, i=i):
            fs = pl.ds(pl.multiple_of(t * ft, ft), ft)
            g = jnp.dot(xg, wg[cs, fs], preferred_element_type=F32)
            u = jnp.dot(xg, wu[cs, fs], preferred_element_type=F32)
            if i:
                g = g + accg[:, fs]
                u = u + accu[:, fs]
            accg[:, fs] = g
            accu[:, fs] = u
            return carry

        lax.fori_loop(0, FW // ft, step, 0)
    r = lax.rsqrt(square / D + 1e-5)

    def act(t, carry):
        fs = pl.ds(pl.multiple_of(t * ft, ft), ft)
        g = accg[:, fs] * r
        u = accu[:, fs] * r
        inner[:, fs] = (g / (1.0 + jnp.exp(-g)) * u).astype(BF)
        return carry

    lax.fori_loop(0, FW // ft, act, 0)
    for cp in rs_copies:
        cp.wait_send()
    wcopies[-1].wait()
    r2_copies = scatter(wd, inner, r2_s, r2_r)
    for i in range(CHUNKS):
        cs = pl.ds(i * CW, CW)
        out[:, cs] = (gath[my_rows, cs].astype(F32) + reduced(i, r2_copies)).astype(BF)

    for cp in ag_copies + r2_copies:
        cp.wait_send()
    for t in range(2):
        @pl.when(j < J - 1)
        def _():
            z_copy(b, t).wait_send()

        @pl.when(c == 0)
        def _():
            d_copy(b, t).wait_send()

    def drain(s, carry):
        slot = 2 * (j - 1 - s) + c
        for t in range(2):
            @pl.when(j < J - 1)
            def _():
                z_copy(slot, t).wait_send()

            d_copy(slot, t).wait_send()
        return carry

    lax.fori_loop(0, j, drain, 0)


def solution(mesh):
    H = mesh.shape["head"]
    B = mesh.shape["blk"]

    def local(hid, q, k, v, wo, gain, wg, wu, wd):
        T, D = hid.shape
        R = T * H
        QW = q.shape[1] // H
        KW = k.shape[1] // H
        FW = wg.shape[1]
        vm = pl.BlockSpec(memory_space=pltpu.VMEM)
        hbm = pl.BlockSpec(memory_space=pl.ANY)
        dma = pltpu.SemaphoreType.DMA
        return pl.pallas_call(
            functools.partial(kernel, H, B),
            out_shape=jax.ShapeDtypeStruct((T, D), BF),
            in_specs=[vm] * 5 + [hbm] * 4,
            out_specs=vm,
            scratch_shapes=[
                pltpu.VMEM(wo.shape, BF),
                pltpu.VMEM(wg.shape, BF),
                pltpu.VMEM(wu.shape, BF),
                pltpu.VMEM(wd.shape, BF),
                pltpu.VMEM((R, QW), BF),
                pltpu.VMEM((B, 2, R, KW), BF),
                pltpu.VMEM((R, QW), BF),
                pltpu.VMEM((R, D), BF),
                pltpu.VMEM((H - 1, T, D), BF),
                pltpu.VMEM((R, D), BF),
                pltpu.VMEM((R, FW), F32),
                pltpu.VMEM((R, FW), F32),
                pltpu.VMEM((R, FW), BF),
                dma((2 + 2 * CHUNKS,)),
                dma((3,)),
                dma((H - 1, 3)), dma((H - 1, 3)),
                dma((B, 2)), dma((B, 2)),
                dma((B, 2)), dma((B, 2)),
                dma((H - 1, CHUNKS)), dma((H - 1, CHUNKS)),
                dma((H - 1, CHUNKS)), dma((H - 1, CHUNKS)),
                dma((H - 1, CHUNKS)), dma((H - 1, CHUNKS)),
            ],
            compiler_params=pltpu.CompilerParams(
                collective_id=0, has_side_effects=True, vmem_limit_bytes=67_043_328
            ),
        )(hid, q, k, v, gain.reshape(1, -1), wo, wg, wu, wd)

    rows = P(("blk", "head"), None)
    return jax.shard_map(
        local,
        mesh=mesh,
        in_specs=(rows, rows, rows, rows, P("head", None), P(), P(None, "head"), P(None, "head"), P("head", None)),
        out_specs=rows,
        check_vma=False,
    )
```

```python
import functools

import jax
import jax.numpy as jnp
from jax import lax
from jax.experimental import pallas as pl
from jax.experimental.pallas import tpu as pltpu
from jax.sharding import PartitionSpec as P

HEADS = 16
KV_HEADS = 8
HEAD_DIM = 128
CHUNKS = 4
MESH = pl.DeviceIdType.MESH
BF = jnp.bfloat16
F32 = jnp.float32


def tile_of(n, most=256):
    t = most
    while n % t:
        t -= 128
    return t


def remote(src, dst, send, recv, axis, index):
    return pltpu.make_async_remote_copy(
        src_ref=src, dst_ref=dst, send_sem=send, recv_sem=recv,
        device_id={axis: index}, device_id_type=MESH,
    )


def kernel(
    H, B,
    hid, q_in, k_in, v_in, gain, wo_h, wg_h, wu_h, wd_h,
    out,
    wo, wg, wu, wd, qb, kv, att, part, rs, gath, accg, accu, inner,
    w_sem, loc_sem, a_s, a_r, z_s, z_r, d_s, d_r, rs_s, rs_r, ag_s, ag_r, r2_s, r2_r,
):
    h = lax.axis_index("head")
    b = lax.axis_index("blk")
    J = B // 2
    j = b // 2
    c = b % 2
    partner = b + 1 - 2 * c
    T = hid.shape[0]
    D = hid.shape[1]
    R = T * H
    QW = qb.shape[1]
    KW = kv.shape[3]
    nh = QW // HEAD_DIM
    ratio = HEADS // KV_HEADS
    CW = D // CHUNKS
    FW = wg.shape[1]

    wcopies = [pltpu.make_async_copy(wo_h, wo, w_sem.at[0])]
    for i in range(CHUNKS):
        rows = pl.ds(i * CW, CW)
        wcopies.append(pltpu.make_async_copy(wg_h.at[rows], wg.at[rows], w_sem.at[1 + 2 * i]))
        wcopies.append(pltpu.make_async_copy(wu_h.at[rows], wu.at[rows], w_sem.at[2 + 2 * i]))
    wcopies.append(pltpu.make_async_copy(wd_h, wd, w_sem.at[1 + 2 * CHUNKS]))
    for w in wcopies:
        w.start()

    barrier = pltpu.get_barrier_semaphore()
    for d in range(1, H):
        pl.semaphore_signal(barrier, inc=1, device_id={"head": lax.rem(h + d, H)}, device_id_type=MESH)
    for d in range(1, J):
        pl.semaphore_signal(barrier, inc=1, device_id={"blk": lax.rem(b + 2 * d, B)}, device_id_type=MESH)
    pl.semaphore_signal(barrier, inc=1, device_id={"blk": partner}, device_id_type=MESH)
    pl.semaphore_wait(barrier, H - 1 + J - 1 + 1)

    my_rows = pl.ds(pl.multiple_of(h * T, T), T)

    def cols(p, w):
        return pl.ds(pl.multiple_of(p * w, w), w)

    a_copies = []
    for t, (src, dst, w) in enumerate(
        ((k_in, kv.at[b, 0], KW), (v_in, kv.at[b, 1], KW), (q_in, qb, QW))
    ):
        for d in range(1, H):
            p = lax.rem(h + d, H)
            cp = remote(
                src.at[:, cols(p, w)], dst.at[my_rows, :],
                a_s.at[d - 1, t], a_r.at[d - 1, t], "head", p,
            )
            cp.start()
            a_copies.append((t, cp))
        lc = pltpu.make_async_copy(src.at[:, cols(h, w)], dst.at[my_rows, :], loc_sem.at[t])
        lc.start()
        a_copies.append((t, lc))

    def wait_in(t):
        for tt, cp in a_copies:
            if tt == t:
                cp.wait()

    def z_copy(slot, t):
        return remote(
            kv.at[slot, t], kv.at[slot, t], z_s.at[slot, t], z_r.at[slot, t],
            "blk", lax.rem(b + 2, B),
        )

    def d_copy(slot, t):
        return remote(
            kv.at[slot, t], kv.at[slot, t], d_s.at[slot, t], d_r.at[slot, t], "blk", partner
        )

    for t in range(2):
        wait_in(t)

        @pl.when(j < J - 1)
        def _():
            z_copy(b, t).start()

        @pl.when(c == 0)
        def _():
            d_copy(b, t).start()

    wait_in(2)

    mq = lambda n: slice(n * HEAD_DIM, (n + 1) * HEAD_DIM)
    ml = lambda n: slice((nh + n) * HEAD_DIM, (nh + n + 1) * HEAD_DIM)
    scale = HEAD_DIM ** (-0.5)

    def absorb(slot, first):
        for n in range(nh):
            g = n // ratio
            s = lax.dot_general(
                qb[:, mq(n)], kv[slot, 0, :, mq(g)],
                (((1,), (1,)), ((), ())), preferred_element_type=F32,
            ) * scale
            if first:
                qi = lax.broadcasted_iota(jnp.int32, s.shape, 0)
                ki = lax.broadcasted_iota(jnp.int32, s.shape, 1)
                s = jnp.where(ki <= qi, s, -1e30)
            top = jnp.max(s, axis=1, keepdims=True)
            if not first:
                old = accu[:, mq(n)][:, :1]
                top = jnp.maximum(top, old)
            e = jnp.exp(s - top)
            tot = jnp.sum(e, axis=1, keepdims=True)
            pv = jnp.dot(e.astype(BF), kv[slot, 1, :, mq(g)], preferred_element_type=F32)
            if not first:
                f = jnp.exp(old - top)
                tot = tot + accu[:, ml(n)][:, :1] * f
                pv = pv + accg[:, mq(n)] * f
            accu[:, mq(n)] = jnp.broadcast_to(top, (R, HEAD_DIM))
            accu[:, ml(n)] = jnp.broadcast_to(tot, (R, HEAD_DIM))
            accg[:, mq(n)] = pv

    absorb(b, True)

    @pl.when(c == 1)
    def _():
        for t in range(2):
            d_copy(b - 1, t).wait_recv()
        absorb(b - 1, False)

    def chain(s, carry):
        slot = 2 * (j - 1 - s) + c
        other = 2 * (j - 1 - s) + 1 - c
        for t in range(2):
            z_copy(slot, t).wait_recv()

            @pl.when(j < J - 1)
            def _():
                z_copy(slot, t).start()

            d_copy(slot, t).start()
        absorb(slot, False)
        for t in range(2):
            d_copy(other, t).wait_recv()
        absorb(other, False)
        return carry

    lax.fori_loop(0, j, chain, 0)

    for n in range(nh):
        att[:, mq(n)] = (accg[:, mq(n)] / accu[:, ml(n)]).astype(BF)

    square_ring = H == 4
    nx = h + 1 - 2 * (h % 2)
    ny = lax.rem(h + H // 2, H)
    dg = H - 1 - h
    HW = CW // 2

    def rows_of(p):
        return pl.ds(pl.multiple_of(p * T, T), T)

    def halves(i):
        return pl.ds(i * CW, HW), pl.ds(i * CW + HW, HW)

    def scatter(w_ref, x_ref, send, recv):
        copies = {}
        ct = tile_of(CW)
        for i in range(CHUNKS):
            def step(t, carry):
                cs = pl.ds(pl.multiple_of(i * CW + t * ct, ct), ct)
                part[:, cs] = jnp.dot(
                    x_ref[...], w_ref[:, cs], preferred_element_type=F32
                ).astype(BF)
                return carry

            lax.fori_loop(0, CW // ct, step, 0)
            if square_ring:
                ha, hb = halves(i)
                plan = ((1, dg, ha, 0, nx), (1, dg, hb, 1, ny), (0, nx, ha, 2, nx), (0, ny, hb, 3, ny))
            else:
                cs = pl.ds(i * CW, CW)
                plan = [(d - 1, lax.rem(h + d, H), cs, d - 1, lax.rem(h + d, H)) for d in range(1, H)]
            for place, block, cs, sem, to in plan:
                cp = remote(
                    part.at[rows_of(block), cs], rs.at[place, :, cs],
                    send.at[sem, i], recv.at[sem, i], "head", to,
                )
                cp.start()
                copies[sem, i] = cp
        return copies

    def combine(i, copies, send, recv):
        if not square_ring:
            return
        ha, hb = halves(i)
        for cs, sem, to in ((ha, 0, ny), (hb, 1, nx)):
            copies[sem, i].wait_recv()
            blk_rows = rows_of(to)
            part[blk_rows, cs] = (
                part[blk_rows, cs].astype(F32) + rs[1, :, cs].astype(F32)
            ).astype(BF)
            cp = remote(
                part.at[blk_rows, cs], rs.at[2, :, cs],
                send.at[4 + sem, i], recv.at[4 + sem, i], "head", to,
            )
            cp.start()
            copies[4 + sem, i] = cp

    def reduced(i, copies):
        cs = pl.ds(i * CW, CW)
        sems = (2, 3, 4, 5) if square_ring else range(H - 1)
        for sem in sems:
            copies[sem, i].wait_recv()
        total = part[my_rows, cs].astype(F32)
        for place in (0, 2) if square_ring else range(H - 1):
            total = total + rs[place, :, cs].astype(F32)
        return total

    wcopies[0].wait()
    rs_copies = scatter(wo, att, rs_s, rs_r)
    ag_copies = {}

    def spread(rows, cs, sem, i, to):
        cp = remote(
            gath.at[rows, cs], gath.at[rows, cs],
            ag_s.at[sem, i], ag_r.at[sem, i], "head", to,
        )
        cp.start()
        ag_copies[sem, i] = cp

    for i in range(CHUNKS + 1):
        if i < CHUNKS:
            combine(i, rs_copies, rs_s, rs_r)
        if i:
            cs = pl.ds((i - 1) * CW, CW)
            gath[my_rows, cs] = (hid[:, cs].astype(F32) + reduced(i - 1, rs_copies)).astype(BF)
            for sem, to in enumerate(
                (nx, ny) if square_ring else [lax.rem(h + d, H) for d in range(1, H)]
            ):
                spread(my_rows, cs, sem, i - 1, to)

    ft = tile_of(FW)
    square = jnp.zeros((R, 1), F32)
    for i in range(CHUNKS + 1):
        if i < CHUNKS and square_ring:
            ha, hb = halves(i)
            ag_copies[0, i].wait_recv()
            spread(rows_of(nx), ha, 2, i, ny)
            ag_copies[1, i].wait_recv()
            spread(rows_of(ny), hb, 3, i, nx)
        if i == 0:
            continue
        k = i - 1
        cs = pl.ds(k * CW, CW)
        for sem in (2, 3) if square_ring else range(H - 1):
            ag_copies[sem, k].wait_recv()
        wcopies[1 + 2 * k].wait()
        wcopies[2 + 2 * k].wait()
        x = gath[:, cs].astype(F32)
        square = square + jnp.sum(x * x, axis=1, keepdims=True)
        xg = (x * gain[:, cs]).astype(BF)

        def step(t, carry, xg=xg, cs=cs, k=k):
            fs = pl.ds(pl.multiple_of(t * ft, ft), ft)
            g = jnp.dot(xg, wg[cs, fs], preferred_element_type=F32)
            u = jnp.dot(xg, wu[cs, fs], preferred_element_type=F32)
            if k:
                g = g + accg[:, fs]
                u = u + accu[:, fs]
            accg[:, fs] = g
            accu[:, fs] = u
            return carry

        lax.fori_loop(0, FW // ft, step, 0)
    r = lax.rsqrt(square / D + 1e-5)

    def act(t, carry):
        fs = pl.ds(pl.multiple_of(t * ft, ft), ft)
        g = accg[:, fs] * r
        u = accu[:, fs] * r
        inner[:, fs] = (g / (1.0 + jnp.exp(-g)) * u).astype(BF)
        return carry

    lax.fori_loop(0, FW // ft, act, 0)
    for cp in rs_copies.values():
        cp.wait_send()
    wcopies[-1].wait()
    r2_copies = scatter(wd, inner, r2_s, r2_r)
    for i in range(CHUNKS + 1):
        if i < CHUNKS:
            combine(i, r2_copies, r2_s, r2_r)
        if i:
            cs = pl.ds((i - 1) * CW, CW)
            out[:, cs] = (gath[my_rows, cs].astype(F32) + reduced(i - 1, r2_copies)).astype(BF)

    for cp in (*ag_copies.values(), *r2_copies.values()):
        cp.wait_send()
    for t in range(2):
        @pl.when(j < J - 1)
        def _():
            z_copy(b, t).wait_send()

        @pl.when(c == 0)
        def _():
            d_copy(b, t).wait_send()

    def drain(s, carry):
        slot = 2 * (j - 1 - s) + c
        for t in range(2):
            @pl.when(j < J - 1)
            def _():
                z_copy(slot, t).wait_send()

            d_copy(slot, t).wait_send()
        return carry

    lax.fori_loop(0, j, drain, 0)


def solution(mesh):
    H = mesh.shape["head"]
    B = mesh.shape["blk"]

    def local(hid, q, k, v, wo, gain, wg, wu, wd):
        T, D = hid.shape
        R = T * H
        QW = q.shape[1] // H
        KW = k.shape[1] // H
        FW = wg.shape[1]
        vm = pl.BlockSpec(memory_space=pltpu.VMEM)
        hbm = pl.BlockSpec(memory_space=pl.ANY)
        dma = pltpu.SemaphoreType.DMA
        return pl.pallas_call(
            functools.partial(kernel, H, B),
            out_shape=jax.ShapeDtypeStruct((T, D), BF),
            in_specs=[vm] * 5 + [hbm] * 4,
            out_specs=vm,
            scratch_shapes=[
                pltpu.VMEM(wo.shape, BF),
                pltpu.VMEM(wg.shape, BF),
                pltpu.VMEM(wu.shape, BF),
                pltpu.VMEM(wd.shape, BF),
                pltpu.VMEM((R, QW), BF),
                pltpu.VMEM((B, 2, R, KW), BF),
                pltpu.VMEM((R, QW), BF),
                pltpu.VMEM((R, D), BF),
                pltpu.VMEM((H - 1, T, D), BF),
                pltpu.VMEM((R, D), BF),
                pltpu.VMEM((R, FW), F32),
                pltpu.VMEM((R, FW), F32),
                pltpu.VMEM((R, FW), BF),
                dma((2 + 2 * CHUNKS,)),
                dma((3,)),
                dma((H - 1, 3)), dma((H - 1, 3)),
                dma((B, 2)), dma((B, 2)),
                dma((B, 2)), dma((B, 2)),
                dma((max(H - 1, 6), CHUNKS)), dma((max(H - 1, 6), CHUNKS)),
                dma((max(H - 1, 6), CHUNKS)), dma((max(H - 1, 6), CHUNKS)),
                dma((max(H - 1, 6), CHUNKS)), dma((max(H - 1, 6), CHUNKS)),
            ],
            compiler_params=pltpu.CompilerParams(
                collective_id=0, has_side_effects=True, vmem_limit_bytes=67_043_328
            ),
        )(hid, q, k, v, gain.reshape(1, -1), wo, wg, wu, wd)

    rows = P(("blk", "head"), None)
    return jax.shard_map(
        local,
        mesh=mesh,
        in_specs=(rows, rows, rows, rows, P("head", None), P(), P(None, "head"), P(None, "head"), P("head", None)),
        out_specs=rows,
        check_vma=False,
    )
```

```python
import functools

import jax
import jax.numpy as jnp
from jax import lax
from jax.experimental import pallas as pl
from jax.experimental.pallas import tpu as pltpu
from jax.sharding import PartitionSpec as P

HEADS = 16
KV_HEADS = 8
HEAD_DIM = 128
CHUNKS = 4
AHEAD = 2
MESH = pl.DeviceIdType.MESH
BF = jnp.bfloat16
F32 = jnp.float32


def tile_of(n, most=256):
    t = most
    while n % t:
        t -= 128
    return t


def remote(src, dst, send, recv, axis, index):
    return pltpu.make_async_remote_copy(
        src_ref=src, dst_ref=dst, send_sem=send, recv_sem=recv,
        device_id={axis: index}, device_id_type=MESH,
    )


def kernel(
    H, B,
    hid, q_in, k_in, v_in, gain, wo_h, wg_h, wu_h, wd_h,
    out,
    wo, wg, wu, wd, qb, kv, att, part, rs, gath, accg, accu, inner,
    w_sem, loc_sem, a_s, a_r, z_s, z_r, d_s, d_r, rs_s, rs_r, ag_s, ag_r, r2_s, r2_r,
):
    h = lax.axis_index("head")
    b = lax.axis_index("blk")
    J = B // 2
    j = b // 2
    c = b % 2
    partner = b + 1 - 2 * c
    T = hid.shape[0]
    D = hid.shape[1]
    R = T * H
    QW = qb.shape[1]
    KW = kv.shape[3]
    nh = QW // HEAD_DIM
    ratio = HEADS // KV_HEADS
    CW = D // CHUNKS
    FW = wg.shape[1]

    wcopies = [pltpu.make_async_copy(wo_h, wo, w_sem.at[0])]
    for i in range(CHUNKS):
        rows = pl.ds(i * CW, CW)
        wcopies.append(pltpu.make_async_copy(wg_h.at[rows], wg.at[rows], w_sem.at[1 + 2 * i]))
        wcopies.append(pltpu.make_async_copy(wu_h.at[rows], wu.at[rows], w_sem.at[2 + 2 * i]))
    wcopies.append(pltpu.make_async_copy(wd_h, wd, w_sem.at[1 + 2 * CHUNKS]))
    barrier = pltpu.get_barrier_semaphore()
    for d in range(1, H):
        pl.semaphore_signal(barrier, inc=1, device_id={"head": lax.rem(h + d, H)}, device_id_type=MESH)

    @pl.when(j > 0)
    def _():
        pl.semaphore_signal(barrier, inc=1, device_id={"blk": lax.rem(b + B - 2, B)}, device_id_type=MESH)

    @pl.when(j < J - 1)
    def _():
        pl.semaphore_signal(barrier, inc=1, device_id={"blk": lax.rem(b + 2, B)}, device_id_type=MESH)

    pl.semaphore_signal(barrier, inc=1, device_id={"blk": partner}, device_id_type=MESH)
    pl.semaphore_wait(barrier, H + jnp.minimum(j, 1) + jnp.minimum(J - 1 - j, 1))

    my_rows = pl.ds(pl.multiple_of(h * T, T), T)

    def cols(p, w):
        return pl.ds(pl.multiple_of(p * w, w), w)

    a_copies = []
    for t, (src, dst, w) in enumerate(
        ((k_in, kv.at[b, 0], KW), (v_in, kv.at[b, 1], KW), (q_in, qb, QW))
    ):
        for d in range(1, H):
            p = lax.rem(h + d, H)
            cp = remote(
                src.at[:, cols(p, w)], dst.at[my_rows, :],
                a_s.at[d - 1, t], a_r.at[d - 1, t], "head", p,
            )
            cp.start()
            a_copies.append((t, cp))
        lc = pltpu.make_async_copy(src.at[:, cols(h, w)], dst.at[my_rows, :], loc_sem.at[t])
        lc.start()
        a_copies.append((t, lc))

    def wait_in(t):
        for tt, cp in a_copies:
            if tt == t:
                cp.wait()

    def z_copy(slot, t):
        return remote(
            kv.at[slot, t], kv.at[slot, t], z_s.at[slot, t], z_r.at[slot, t],
            "blk", lax.rem(b + 2, B),
        )

    def d_copy(slot, t):
        return remote(
            kv.at[slot, t], kv.at[slot, t], d_s.at[slot, t], d_r.at[slot, t], "blk", partner
        )

    for t in range(2):
        wait_in(t)

        @pl.when(j < J - 1)
        def _():
            z_copy(b, t).start()

        @pl.when(c == 0)
        def _():
            d_copy(b, t).start()

    wait_in(2)
    for w in wcopies:
        w.start()

    mq = lambda n: slice(n * HEAD_DIM, (n + 1) * HEAD_DIM)
    ml = lambda n: slice((nh + n) * HEAD_DIM, (nh + n + 1) * HEAD_DIM)
    scale = HEAD_DIM ** (-0.5)

    def absorb(slot, first):
        for n in range(nh):
            g = n // ratio
            s = lax.dot_general(
                qb[:, mq(n)], kv[slot, 0, :, mq(g)],
                (((1,), (1,)), ((), ())), preferred_element_type=F32,
            ) * scale
            if first:
                qi = lax.broadcasted_iota(jnp.int32, s.shape, 0)
                ki = lax.broadcasted_iota(jnp.int32, s.shape, 1)
                s = jnp.where(ki <= qi, s, -1e30)
            top = jnp.max(s, axis=1, keepdims=True)
            if not first:
                old = accu[:, mq(n)][:, :1]
                top = jnp.maximum(top, old)
            e = jnp.exp(s - top)
            tot = jnp.sum(e, axis=1, keepdims=True)
            pv = jnp.dot(e.astype(BF), kv[slot, 1, :, mq(g)], preferred_element_type=F32)
            if not first:
                f = jnp.exp(old - top)
                tot = tot + accu[:, ml(n)][:, :1] * f
                pv = pv + accg[:, mq(n)] * f
            accu[:, mq(n)] = jnp.broadcast_to(top, (R, HEAD_DIM))
            accu[:, ml(n)] = jnp.broadcast_to(tot, (R, HEAD_DIM))
            accg[:, mq(n)] = pv

    absorb(b, True)

    @pl.when(c == 1)
    def _():
        for t in range(2):
            d_copy(b - 1, t).wait_recv()
        absorb(b - 1, False)

    def chain(s, carry):
        slot = 2 * (j - 1 - s) + c
        other = 2 * (j - 1 - s) + 1 - c
        for t in range(2):
            z_copy(slot, t).wait_recv()

            @pl.when(j < J - 1)
            def _():
                z_copy(slot, t).start()

            d_copy(slot, t).start()
        absorb(slot, False)
        for t in range(2):
            d_copy(other, t).wait_recv()
        absorb(other, False)
        return carry

    lax.fori_loop(0, j, chain, 0)

    for n in range(nh):
        att[:, mq(n)] = (accg[:, mq(n)] / accu[:, ml(n)]).astype(BF)

    square_ring = H == 4
    nx = h + 1 - 2 * (h % 2)
    ny = lax.rem(h + H // 2, H)
    dg = H - 1 - h
    HW = CW // 2

    def rows_of(p):
        return pl.ds(pl.multiple_of(p * T, T), T)

    def halves(i):
        return pl.ds(i * CW, HW), pl.ds(i * CW + HW, HW)

    def scatter(w_ref, x_ref, send, recv):
        copies = {}
        ct = tile_of(CW)
        for i in range(CHUNKS):
            def step(t, carry):
                cs = pl.ds(pl.multiple_of(i * CW + t * ct, ct), ct)
                part[:, cs] = jnp.dot(
                    x_ref[...], w_ref[:, cs], preferred_element_type=F32
                ).astype(BF)
                return carry

            lax.fori_loop(0, CW // ct, step, 0)
            if square_ring:
                ha, hb = halves(i)
                plan = ((1, dg, ha, 0, nx), (1, dg, hb, 1, ny), (0, nx, ha, 2, nx), (0, ny, hb, 3, ny))
            else:
                cs = pl.ds(i * CW, CW)
                plan = [(d - 1, lax.rem(h + d, H), cs, d - 1, lax.rem(h + d, H)) for d in range(1, H)]
            for place, block, cs, sem, to in plan:
                cp = remote(
                    part.at[rows_of(block), cs], rs.at[place, :, cs],
                    send.at[sem, i], recv.at[sem, i], "head", to,
                )
                cp.start()
                copies[sem, i] = cp
        return copies

    def combine(i, copies, send, recv):
        if not square_ring:
            return
        ha, hb = halves(i)
        for cs, sem, to in ((ha, 0, ny), (hb, 1, nx)):
            copies[sem, i].wait_recv()
            blk_rows = rows_of(to)
            part[blk_rows, cs] = (
                part[blk_rows, cs].astype(F32) + rs[1, :, cs].astype(F32)
            ).astype(BF)
            cp = remote(
                part.at[blk_rows, cs], rs.at[2, :, cs],
                send.at[4 + sem, i], recv.at[4 + sem, i], "head", to,
            )
            cp.start()
            copies[4 + sem, i] = cp

    def reduced(i, copies):
        cs = pl.ds(i * CW, CW)
        sems = (2, 3, 4, 5) if square_ring else range(H - 1)
        for sem in sems:
            copies[sem, i].wait_recv()
        total = part[my_rows, cs].astype(F32)
        for place in (0, 2) if square_ring else range(H - 1):
            total = total + rs[place, :, cs].astype(F32)
        return total

    wcopies[0].wait()
    rs_copies = scatter(wo, att, rs_s, rs_r)
    ag_copies = {}

    def spread(rows, cs, sem, i, to):
        cp = remote(
            gath.at[rows, cs], gath.at[rows, cs],
            ag_s.at[sem, i], ag_r.at[sem, i], "head", to,
        )
        cp.start()
        ag_copies[sem, i] = cp

    def spread_own(i):
        for sem, to in enumerate(
            (nx, ny) if square_ring else [lax.rem(h + d, H) for d in range(1, H)]
        ):
            spread(my_rows, pl.ds(i * CW, CW), sem, i, to)

    for i in range(CHUNKS + 1):
        if i < CHUNKS:
            combine(i, rs_copies, rs_s, rs_r)
        if i:
            cs = pl.ds((i - 1) * CW, CW)
            gath[my_rows, cs] = (hid[:, cs].astype(F32) + reduced(i - 1, rs_copies)).astype(BF)
            if i <= AHEAD or not square_ring:
                spread_own(i - 1)

    ft = tile_of(FW)
    square = jnp.zeros((R, 1), F32)
    for i in range(CHUNKS + 1):
        if i < CHUNKS and square_ring:
            ha, hb = halves(i)
            ag_copies[0, i].wait_recv()
            spread(rows_of(nx), ha, 2, i, ny)
            ag_copies[1, i].wait_recv()
            spread(rows_of(ny), hb, 3, i, nx)
            if i + AHEAD < CHUNKS:
                spread_own(i + AHEAD)
        if i == 0:
            continue
        k = i - 1
        cs = pl.ds(k * CW, CW)
        for sem in (2, 3) if square_ring else range(H - 1):
            ag_copies[sem, k].wait_recv()
        wcopies[1 + 2 * k].wait()
        wcopies[2 + 2 * k].wait()
        x = gath[:, cs].astype(F32)
        square = square + jnp.sum(x * x, axis=1, keepdims=True)
        xg = (x * gain[:, cs]).astype(BF)

        def step(t, carry, xg=xg, cs=cs, k=k):
            fs = pl.ds(pl.multiple_of(t * ft, ft), ft)
            g = jnp.dot(xg, wg[cs, fs], preferred_element_type=F32)
            u = jnp.dot(xg, wu[cs, fs], preferred_element_type=F32)
            if k:
                g = g + accg[:, fs]
                u = u + accu[:, fs]
            accg[:, fs] = g
            accu[:, fs] = u
            return carry

        lax.fori_loop(0, FW // ft, step, 0)
    r = lax.rsqrt(square / D + 1e-5)

    def act(t, carry):
        fs = pl.ds(pl.multiple_of(t * ft, ft), ft)
        g = accg[:, fs] * r
        u = accu[:, fs] * r
        inner[:, fs] = (g / (1.0 + jnp.exp(-g)) * u).astype(BF)
        return carry

    lax.fori_loop(0, FW // ft, act, 0)
    for cp in rs_copies.values():
        cp.wait_send()
    wcopies[-1].wait()
    r2_copies = scatter(wd, inner, r2_s, r2_r)
    for i in range(CHUNKS + 1):
        if i < CHUNKS:
            combine(i, r2_copies, r2_s, r2_r)
        if i:
            cs = pl.ds((i - 1) * CW, CW)
            out[:, cs] = (gath[my_rows, cs].astype(F32) + reduced(i - 1, r2_copies)).astype(BF)

    for cp in (*ag_copies.values(), *r2_copies.values()):
        cp.wait_send()
    for t in range(2):
        @pl.when(j < J - 1)
        def _():
            z_copy(b, t).wait_send()

        @pl.when(c == 0)
        def _():
            d_copy(b, t).wait_send()

    def drain(s, carry):
        slot = 2 * (j - 1 - s) + c
        for t in range(2):
            @pl.when(j < J - 1)
            def _():
                z_copy(slot, t).wait_send()

            d_copy(slot, t).wait_send()
        return carry

    lax.fori_loop(0, j, drain, 0)


def solution(mesh):
    H = mesh.shape["head"]
    B = mesh.shape["blk"]

    def local(hid, q, k, v, wo, gain, wg, wu, wd):
        T, D = hid.shape
        R = T * H
        QW = q.shape[1] // H
        KW = k.shape[1] // H
        FW = wg.shape[1]
        vm = pl.BlockSpec(memory_space=pltpu.VMEM)
        hbm = pl.BlockSpec(memory_space=pl.ANY)
        dma = pltpu.SemaphoreType.DMA
        return pl.pallas_call(
            functools.partial(kernel, H, B),
            out_shape=jax.ShapeDtypeStruct((T, D), BF),
            in_specs=[vm] * 5 + [hbm] * 4,
            out_specs=vm,
            scratch_shapes=[
                pltpu.VMEM(wo.shape, BF),
                pltpu.VMEM(wg.shape, BF),
                pltpu.VMEM(wu.shape, BF),
                pltpu.VMEM(wd.shape, BF),
                pltpu.VMEM((R, QW), BF),
                pltpu.VMEM((B, 2, R, KW), BF),
                pltpu.VMEM((R, QW), BF),
                pltpu.VMEM((R, D), BF),
                pltpu.VMEM((H - 1, T, D), BF),
                pltpu.VMEM((R, D), BF),
                pltpu.VMEM((R, FW), F32),
                pltpu.VMEM((R, FW), F32),
                pltpu.VMEM((R, FW), BF),
                dma((2 + 2 * CHUNKS,)),
                dma((3,)),
                dma((H - 1, 3)), dma((H - 1, 3)),
                dma((B, 2)), dma((B, 2)),
                dma((B, 2)), dma((B, 2)),
                dma((max(H - 1, 6), CHUNKS)), dma((max(H - 1, 6), CHUNKS)),
                dma((max(H - 1, 6), CHUNKS)), dma((max(H - 1, 6), CHUNKS)),
                dma((max(H - 1, 6), CHUNKS)), dma((max(H - 1, 6), CHUNKS)),
            ],
            compiler_params=pltpu.CompilerParams(
                collective_id=0, has_side_effects=True, vmem_limit_bytes=67_043_328
            ),
        )(hid, q, k, v, gain.reshape(1, -1), wo, wg, wu, wd)

    rows = P(("blk", "head"), None)
    return jax.shard_map(
        local,
        mesh=mesh,
        in_specs=(rows, rows, rows, rows, P("head", None), P(), P(None, "head"), P(None, "head"), P("head", None)),
        out_specs=rows,
        check_vma=False,
    )
```
